32 devices in a mesh: gx: 4 (over y, core), gy: 2 (over x), gz: 4 (over z).
Axes of the slice: x: 2, y: 2, z: 4, core: 2. Of those that a mesh axis runs over, the one named last changes fastest.
Arguments:
- positions: float32 [3, 4, 2, 4, 512], P(None, 'gx', 'gy', 'gz'), may hold values from 0 to 1
- velocities: float32 [3, 4, 2, 4, 512], P(None, 'gx', 'gy', 'gz'), may hold values from -6 to 6
- charges: float32 [4, 2, 4, 512], P('gx', 'gy', 'gz'), may hold values from -5 to 5
- cluster_atoms: int32 [4, 2, 4, 768], P('gx', 'gy', 'gz'), may hold values from 0 to 512, as said below
- pair_list: int32 [3, 4, 2, 4, 256], P(None, 'gx', 'gy', 'gz'), may hold values from 0 to 124, as said below
Outputs:
- new_positions: float32 [3, 4, 2, 4, 512], P(None, 'gx', 'gy', 'gz')
- new_velocities: float32 [3, 4, 2, 4, 512], P(None, 'gx', 'gy', 'gz')
- last_forces: float32 [3, 4, 2, 4, 512], P(None, 'gx', 'gy', 'gz')
The draws below stay inside these ranges and needn't reach their ends.
Inputs may be any that keep to these rules, and one draw needn't show every extreme that they name: `cluster_atoms`: on every domain each atom index below 512 stands in exactly one slot; all other slots hold 512, meaning empty. `pair_list`: row 0 and row 1 lie in 0 to 5, row 2 in 0 to 124; on every domain each of the 125 shift indices appears in at least 2 listed pairs.
All inputs are finite; a program needn't handle non-finite values.
Results may differ from the reference program's by a relative error of at most 0.0001.
Values sent between devices are 32-bit elements; how exact they have to be, the bound alone decides.
A program may use at most 64 MiB of HBM per device.

```python
import jax
import jax.numpy as jnp
from jax import lax

CLUSTER = 128
A_DEV = 512
CL_DEV = 6
PAIRS_DEV = 256
STEPS = 2
N_GX = 4
N_GY = 2
N_GZ = 4


def draw_cluster_atoms(key, part):
    device_count = N_GX * N_GY * N_GZ
    slot_count = CL_DEV * CLUSTER

    def per_device(device_key):
        shuffled = jax.random.permutation(device_key, jnp.arange(slot_count, dtype=jnp.int32))
        return jnp.minimum(shuffled, A_DEV).astype(jnp.int32)
    tables = jax.vmap(per_device)(jax.random.split(jax.random.fold_in(key, 11), device_count))
    return tables.reshape(N_GX, N_GY, N_GZ, slot_count)


def draw_pair_list(key, part):
    device_count = N_GX * N_GY * N_GZ
    pair_count = PAIRS_DEV
    covered = 125 * (pair_count // 125)

    def per_device(device_key):
        sub_keys = jax.random.split(device_key, 4)
        ordinal = jnp.arange(pair_count, dtype=jnp.int32)
        extra_shift = jax.random.randint(sub_keys[0], (pair_count,), 0, 125, dtype=jnp.int32)
        shift_index = jnp.where(ordinal < covered, ordinal % 125, extra_shift)
        shift_index = jax.random.permutation(sub_keys[1], shift_index)
        left_cluster = jax.random.randint(sub_keys[2], (pair_count,), 0, CL_DEV, dtype=jnp.int32)
        right_cluster = jax.random.randint(sub_keys[3], (pair_count,), 0, CL_DEV, dtype=jnp.int32)
        return jnp.stack([left_cluster, right_cluster, shift_index])
    pair_rows = jax.vmap(per_device)(jax.random.split(jax.random.fold_in(key, 23), device_count))
    return jnp.transpose(pair_rows, (1, 0, 2)).reshape(3, N_GX, N_GY, N_GZ, pair_count).astype(jnp.int32)


def block_levels(own_key, shape, cuts, smallest, largest):
    factor_of = 1.0
    for position, blocks in cuts:
        steps = jax.random.uniform(jax.random.fold_in(jax.random.fold_in(own_key, 6), position), (blocks,), jnp.float32, smallest / len(cuts), largest / len(cuts))
        factor_of = factor_of * jnp.repeat(jnp.exp(steps), shape[position] // blocks).reshape((-1,) + (1,) * (len(shape) - 1 - position))
    return factor_of


def noise(key, shape, spread, bound, pieces=(), held_as=jnp.bfloat16):
    values = jax.random.normal(key, shape, jnp.float32) * spread
    if len(pieces) > 0:
        values = block_levels(key, shape, pieces, -0.22, 0.18) * values
    return jnp.clip(values, min=-bound, max=bound).astype(held_as)


def setup_inputs(seed: int = 0) -> dict:
    splits = jax.random.split(jax.random.key(seed), 6)
    positions = jnp.clip(1.0 * jax.random.uniform(splits[0], (3, N_GX, N_GY, N_GZ, A_DEV), jnp.float32) ** block_levels(splits[0], (3, N_GX, N_GY, N_GZ, A_DEV), ((1, 4), (2, 2), (3, 4)), -0.2, 0.2), 0.0, 1.0)
    velocities = noise(splits[1], (3, N_GX, N_GY, N_GZ, A_DEV), 1.0, 6.0, ((1, 4), (2, 2), (3, 4)), jnp.float32)
    charges = noise(splits[2], (N_GX, N_GY, N_GZ, A_DEV), 1.0, 5.0, ((0, 4), (1, 2), (2, 4)), jnp.float32)
    cluster_atoms = draw_cluster_atoms(jax.random.fold_in(splits[5], 71), 0)
    pair_list = draw_pair_list(jax.random.fold_in(splits[5], 71), 0)
    return {"positions": positions, "velocities": velocities, "charges": charges, "cluster_atoms": cluster_atoms, "pair_list": pair_list}


CUTOFF_SQ = 4.0
SOFTENING = 0.5
TIME_STEP = 0.02


def pair_terms(left_xyz, left_charge, right_xyz, right_charge):
    separation = left_xyz[:, :, :, None] - right_xyz[:, :, None, :]
    distance_sq = jnp.sum(separation * separation, axis=0)
    window_term = jnp.maximum(1.0 - distance_sq / CUTOFF_SQ, 0.0)
    inverse = 1.0 / (distance_sq + SOFTENING)
    scalar = 2.0 * left_charge[:, :, None] * right_charge[:, None, :] * (
        3.0 * window_term * window_term * inverse / CUTOFF_SQ
        + window_term * window_term * window_term * inverse * inverse)
    pair_force = scalar[None] * separation
    return jnp.sum(pair_force, axis=3), -jnp.sum(pair_force, axis=2)


def forces_of(coords, atom_slots, slot_charge, left_rows, right_rows, offsets):
    device_count = atom_slots.shape[0]
    slot_count = atom_slots.shape[1]
    padded = jnp.concatenate([coords, jnp.zeros((3, device_count, 1), jnp.float32)], axis=2)
    slot_xyz = jnp.take_along_axis(padded, jnp.broadcast_to(atom_slots[None], (3, device_count, slot_count)), axis=2)
    slot_xyz = slot_xyz.reshape(3, device_count * CL_DEV, CLUSTER)
    block_size = 64
    blocks = left_rows.shape[0] // block_size

    def accumulate(carried, block_data):
        rows_left, rows_right, shift_vec = block_data
        left_xyz = slot_xyz[:, rows_left]
        right_xyz = slot_xyz[:, rows_right] + shift_vec[:, :, None]
        left_force, right_force = pair_terms(left_xyz, slot_charge[rows_left], right_xyz, slot_charge[rows_right])
        carried = carried.at[:, rows_left].add(left_force).at[:, rows_right].add(right_force)
        return carried, None

    start = jnp.zeros((3, device_count * CL_DEV, CLUSTER), jnp.float32)
    summed, _ = lax.scan(accumulate, start, (left_rows.reshape(blocks, block_size), right_rows.reshape(blocks, block_size), jnp.transpose(offsets.reshape(3, blocks, block_size), (1, 0, 2))))
    summed = summed.reshape(3, device_count, slot_count)

    def to_atoms(slot_force, slot_index):
        return jnp.zeros((3, A_DEV + 1), jnp.float32).at[:, slot_index].add(slot_force)[:, :A_DEV]

    return jax.vmap(to_atoms, in_axes=(1, 0), out_axes=1)(summed, atom_slots)


def reference(positions, velocities, charges, cluster_atoms, pair_list):
    device_count = N_GX * N_GY * N_GZ
    slot_count = CL_DEV * CLUSTER
    atom_slots = cluster_atoms.reshape(device_count, slot_count).astype(jnp.int32)
    charge_pad = jnp.concatenate([charges.reshape(device_count, A_DEV), jnp.zeros((device_count, 1), jnp.float32)], axis=1)
    slot_charge = jnp.take_along_axis(charge_pad, atom_slots, axis=1).reshape(device_count * CL_DEV, CLUSTER)
    pairs = pair_list.reshape(3, device_count, PAIRS_DEV).astype(jnp.int32)
    device = jnp.arange(device_count, dtype=jnp.int32)[:, None]
    cell_x = device // (N_GY * N_GZ)
    cell_y = (device // N_GZ) % N_GY
    cell_z = device % N_GZ
    shift_index = pairs[2]
    delta_x = shift_index // 25 - 2
    delta_y = (shift_index // 5) % 5 - 2
    delta_z = shift_index % 5 - 2
    source = (((cell_x + delta_x) % N_GX) * N_GY + (cell_y + delta_y) % N_GY) * N_GZ + (cell_z + delta_z) % N_GZ
    left_rows = (device * CL_DEV + pairs[0]).reshape(-1).astype(jnp.int32)
    right_rows = (source * CL_DEV + pairs[1]).reshape(-1).astype(jnp.int32)
    offsets = jnp.stack([delta_x, delta_y, delta_z]).reshape(3, -1).astype(jnp.float32)
    coords = positions.reshape(3, device_count, A_DEV)
    velocity = velocities.reshape(3, device_count, A_DEV)
    forces = jnp.zeros_like(coords)
    for step_index in range(STEPS):
        forces = forces_of(coords, atom_slots, slot_charge, left_rows, right_rows, offsets)
        velocity = velocity + TIME_STEP * forces
        coords = coords + TIME_STEP * velocity
    return coords.reshape(positions.shape), velocity.reshape(positions.shape), forces.reshape(positions.shape)
```

```python
import functools

import jax
import jax.numpy as jnp
from jax import lax
from jax.experimental import pallas as pl
from jax.experimental.pallas import tpu as pltpu
from jax.sharding import PartitionSpec as P

CLUSTER = 128
STEPS = 2
TIME_STEP = 0.02
REACH = 2
SHIFTS = (2 * REACH + 1) ** 3
MESH = pl.DeviceIdType.MESH
AXES = ("gx", "gy", "gz")
VMEM = pl.BlockSpec(memory_space=pltpu.VMEM)
RING = 4
HAND_BLOCKS = 18


def split3(value):
    hi = value.astype(jnp.bfloat16)
    rest = value - hi.astype(jnp.float32)
    mid = rest.astype(jnp.bfloat16)
    lo = (rest - mid.astype(jnp.float32)).astype(jnp.bfloat16)
    return hi, mid, lo


def rounded(value):
    return value.astype(jnp.bfloat16).astype(jnp.float32)


class Zone:
    def __init__(self, sizes):
        self.sizes = sizes
        self.spans = tuple(min(2 * REACH + 1, n) for n in sizes)
        self.lows = tuple(-REACH if n > 2 * REACH else 0 for n in sizes)
        self.count = self.spans[0] * self.spans[1] * self.spans[2]
        self.paired = max(sizes) <= 2 * REACH and sizes[0] % 2 == 0
        self.own = 0
        for low, span in zip(self.lows, self.spans):
            self.own = self.own * span - low
        self.pairs = {z: 0 for z in range(self.count)}
        for t in range(SHIFTS):
            self.pairs[self.place(shift_of(t), 1)] += 2

    def place(self, deltas, turn):
        index = 0
        for axis, (delta, n, span) in enumerate(zip(deltas, self.sizes, self.spans)):
            if axis == 0:
                delta = delta * turn
            if n > 2 * REACH:
                here = delta + REACH
            elif n in (1, 2, 4):
                here = (delta + 2 * n) & (n - 1)
            else:
                here = (delta + 2 * n) % n if isinstance(delta, int) else lax.rem(delta + 2 * n, n)
            index = index * span + here
        return index

    def parts(self, index):
        return (
            index // (self.spans[1] * self.spans[2]),
            (index // self.spans[2]) % self.spans[1],
            index % self.spans[2],
        )

    def odd(self, index):
        return self.paired and self.parts(index)[0] % 2 == 1

    def seen_by_partner(self, index):
        dx, dy, dz = self.parts(index)
        return (((1 - dx) % self.sizes[0]) * self.spans[1] + dy) * self.spans[2] + dz

    def hops(self, index):
        if self.odd(index):
            index = self.seen_by_partner(index)
        near = []
        for n, low, part in zip(self.sizes, self.lows, self.parts(index)):
            off = (part + low) % n
            near.append(min(off, n - off))
        return (near[0] + 1) // 2 + near[1] + near[2]

    def turn(self):
        return 1 - 2 * (lax.axis_index(AXES[0]) % 2) if self.paired else 1

    def peer(self, index, signs):
        out = []
        for axis, n, low, part, sign in zip(AXES, self.sizes, self.lows, self.parts(index), signs):
            out.append((lax.axis_index(axis) + sign * (part + low) + 2 * n) % n)
        return tuple(out)

    def at(self, index):
        return self.peer(index, (self.turn(), 1, 1))

    def sees(self, index):
        turn = self.turn()
        return self.peer(index, (turn if self.odd(index) else -turn, -1, -1))

    def partner(self):
        return (lax.axis_index(AXES[0]) + self.turn(),) + tuple(
            lax.axis_index(axis) for axis in AXES[1:]
        )


class Plan:
    def __init__(self, zone, pair_count):
        extra = pair_count - 2 * SHIFTS
        others = sorted((z for z in range(zone.count) if z != zone.own), key=lambda z: (zone.hops(z), z))
        even = [z for z in others if not zone.odd(z)]
        beside = [z for z in others if zone.odd(z) and zone.hops(z) == 0]
        near = [z for z in even if zone.hops(z) == 1]
        mid = [z for z in even if zone.hops(z) == 2]
        far = [z for z in even if zone.hops(z) > 2]
        twins = lambda zones: [zone.seen_by_partner(z) for z in zones]
        if zone.paired:
            batches = [[zone.own], beside, mid, twins(mid), twins(far), far, twins(near), near]
        else:
            batches = [[zone.own], mid, far, near]
        self.batches = [batch for batch in batches if batch]
        self.order = [z for batch in self.batches for z in batch]
        self.rank = {z: n for n, z in enumerate(self.order)}
        self.first = [self.rank[batch[0]] for batch in self.batches]
        self.size = [len(batch) for batch in self.batches]
        self.second = [zone.odd(batch[0]) and batch != beside for batch in self.batches]
        self.twin = {}
        for n, batch in enumerate(self.batches):
            if self.second[n]:
                m = self.batches.index(twins(batch))
                self.twin[n], self.twin[m] = m, n
        self.direct = [n for n in range(1, len(self.batches)) if not self.second[n]]
        self.starts, self.ends, at = {}, {}, 0
        for z in self.order:
            self.starts[z] = at
            at += zone.pairs[z]
            self.ends[z] = at + extra


def shift_of(t):
    t25 = (t * 5243) >> 17
    t5 = (t * 205) >> 10
    return t25 - 2, t5 - 5 * t25 - 2, t - 5 * t5 - 2


def one_hot(atoms_ref, atom_count):
    slots = atoms_ref.shape[1]
    rows = lax.broadcasted_iota(jnp.int32, (atom_count, slots), 0)
    return jnp.where(rows == atoms_ref[...], 1.0, 0.0).astype(jnp.bfloat16)


def in_work_order(zone, plan, pairs_ref):
    count = pairs_ref.shape[2]
    f32, bf16 = jnp.float32, jnp.bfloat16
    place = zone.place(shift_of(pairs_ref[2]), zone.turn())
    rank = jnp.zeros(place.shape, jnp.int32)
    for n, z in enumerate(plan.order):
        rank = jnp.where(place == z, n, rank)
    key = (rank * count + lax.broadcasted_iota(jnp.int32, place.shape, 1)).astype(f32)
    key_col = jnp.transpose(jnp.broadcast_to(key, (8, count)))[:, 0:1]
    slot = jnp.sum(jnp.where(key_col < key, 1.0, 0.0), axis=0, keepdims=True)
    places = lax.broadcasted_iota(jnp.int32, (count, count), 0).astype(f32)
    hot = jnp.where(places == slot, 1.0, 0.0).astype(bf16)
    rows = [pairs_ref[0], pairs_ref[1], rank, pairs_ref[2]]
    rows = jnp.concatenate([row.astype(f32) for row in rows] + [jnp.zeros((4, count), f32)], axis=0)
    out = lax.dot_general(
        rows.astype(bf16), hot, (((1,), (1,)), ((), ())), preferred_element_type=f32,
    )
    return out.astype(jnp.int32)


def kernel(zone, plan, pairs_ref, x_in, v_in, q_in, atoms_ref, x_out, v_out, f_out,
           first_ref, later_ref, force_ref, land_ref, hand_ref, vel_ref, slot_ref, table_ref,
           shift_ref, a_ref, w_ref, f_ref, push_ref, order_vec_ref, order_ref,
           send_sem, recv_sem, order_sem):
    f32, bf16 = jnp.float32, jnp.bfloat16
    atom_count = x_in.shape[2]
    pair_count = pairs_ref.shape[2]
    slots = atoms_ref.shape[1]
    clusters = slots // CLUSTER
    rows3 = 3 * clusters
    own = zone.own
    barrier = pltpu.get_barrier_semaphore()
    for z in plan.order[1:]:
        pl.semaphore_signal(barrier, 1, device_id=zone.at(z), device_id_type=MESH)

    tile = (8, CLUSTER)
    sub = lax.broadcasted_iota(jnp.int32, tile, 0)
    comp = sub & 3
    upper = sub < 4
    keep_q = jnp.where(comp == 3, 0.0, 1.0)

    def turned(value, by):
        return pltpu.roll(value, by, 0)

    def coords_ref(step):
        return first_ref if step == 0 else later_ref.at[step - 1]

    data = jnp.concatenate(
        [x_in[c] for c in range(3)] + [v_in[c] for c in range(3)]
        + [q_in[...], jnp.zeros((1, atom_count), f32)], axis=0
    )
    stacked = jnp.concatenate(list(split3(data)) + [jnp.zeros(data.shape, bf16)], axis=0)
    out = jnp.dot(stacked, one_hot(atoms_ref, atom_count), preferred_element_type=f32)
    slot = out[0:8] + out[8:16] + out[16:24]
    for k in range(clusters):
        lanes = slice(k * CLUSTER, (k + 1) * CLUSTER)
        for c in range(3):
            first_ref[0, c * clusters + k, :] = slot[c, lanes]
            vel_ref[c * clusters + k, :] = slot[3 + c, lanes]
        first_ref[0, rows3 + k, :] = slot[6, lanes]

    def some(ref, n):
        return ref.at[pl.ds(plan.first[n], plan.size[n])]

    def coords_copy(step, n, z):
        ref = coords_ref(step)
        return pltpu.make_async_remote_copy(
            src_ref=ref.at[0], dst_ref=ref.at[plan.rank[z]],
            send_sem=send_sem.at[2 * step, 0], recv_sem=recv_sem.at[2 * step, n],
            device_id=zone.sees(z), device_id_type=MESH,
        )

    def force_copy(step, n, z):
        return pltpu.make_async_remote_copy(
            src_ref=force_ref.at[step, plan.rank[z]], dst_ref=land_ref.at[step, plan.rank[z]],
            send_sem=send_sem.at[2 * step + 1, 0], recv_sem=recv_sem.at[2 * step + 1, n],
            device_id=zone.at(z), device_id_type=MESH,
        )

    def relay_copy(step, n):
        ref, twin = coords_ref(step), plan.twin[n]
        return pltpu.make_async_remote_copy(
            src_ref=some(ref, n), dst_ref=some(ref, twin),
            send_sem=send_sem.at[2 * step, 1], recv_sem=recv_sem.at[2 * step, twin],
            device_id=zone.partner(), device_id_type=MESH,
        )

    def hand_copy(step, n):
        return pltpu.make_async_remote_copy(
            src_ref=some(force_ref.at[step], n), dst_ref=some(hand_ref.at[step], plan.twin[n]),
            send_sem=send_sem.at[2 * step + 1, 1], recv_sem=recv_sem.at[2 * step + 1, n],
            device_id=zone.partner(), device_id_type=MESH,
        )

    def arrived(ref, sem):
        pltpu.make_async_copy(ref, ref, sem).wait()

    def send_coords(step):
        for n in plan.direct:
            for z in plan.batches[n]:
                coords_copy(step, n, z).start()

    pl.semaphore_wait(barrier, zone.count - 1)
    send_coords(0)

    order_vec_ref[...] = in_work_order(zone, plan, pairs_ref)
    to_scalars = pltpu.make_async_copy(order_vec_ref, order_ref, order_sem)
    to_scalars.start()

    axis_rows = [jnp.where(comp == c, 1.0, 0.0) for c in range(4)]
    for t in range(SHIFTS):
        shift = axis_rows[3]
        for c, delta in enumerate(shift_of(t)):
            if delta:
                shift = shift + float(delta) * axis_rows[c]
        shift_ref[t] = shift

    def receive(step, n, got):
        if n == 0 or n in got:
            return
        got.add(n)
        if plan.second[n]:
            receive(step, plan.twin[n], got)
        arrived(some(coords_ref(step), n), recv_sem.at[2 * step, n])
        if n in plan.twin and not plan.second[n]:
            relay_copy(step, n).start()

    def arrive(step, n, got):
        receive(step, n, got)
        if 2 <= n < len(plan.batches) - 1 and plan.second[n + 1]:
            receive(step, plan.twin[n + 1], got)
        ref = coords_ref(step)
        for r in range(plan.first[n], plan.first[n] + plan.size[n]):
            for k in range(clusters):
                value = first_ref[r, pl.ds(rows3 + k, 1), :]
                for c in range(3):
                    value = jnp.where(comp == c, ref[r, pl.ds(c * clusters + k, 1), :], value)
                table_ref[r * clusters + k] = value

    def weights(value):
        return jnp.where(upper, value, value - rounded(value))

    def own_side(i):
        both = table_ref[i]
        charge = 0.125 * table_ref[i, pl.ds(3, 1), :]
        w_ref[i] = weights(charge * jnp.where(comp == 3, 1.0, both))
        half = 0.5 * both
        high = rounded(half)
        square = half * half
        rest = 1.0 - (square[0:1] + square[1:2] + square[2:3])
        first = rounded(rest)
        second = rounded(rest - first)
        third = rest - first - second
        top = jnp.where(comp == 3, 1.0, high)
        bottom = jnp.where(sub < 3, half - high, 0.0)
        bottom = jnp.where(sub == 3, 1.0, bottom)
        bottom = jnp.where(sub == 4, first, bottom)
        bottom = jnp.where(sub == 5, second, bottom)
        bottom = jnp.where(sub == 6, third, bottom)
        return jnp.concatenate([top, bottom], axis=0)

    def within(value, count):
        return jnp.minimum(jnp.maximum(value, 0), count - 1)

    def prepare(b):
        sides, lefts, dots = [], [], []
        for p in (2 * b, 2 * b + 1):
            i = within(order_ref[0, p], clusters)
            j = within(order_ref[2, p] * clusters + order_ref[1, p], zone.count * clusters)
            t = within(order_ref[3, p], SHIFTS)
            both = table_ref[j]
            charge = table_ref[j, pl.ds(3, 1), :]
            coords = both * keep_q + shift_ref[t]
            w = coords * charge
            sides.append((p, i, j, charge, w))
            lefts.append(weights(0.125 * w))
            square = coords * coords
            norm = -0.25 * (turned(square, 1) + turned(square, 2) + turned(square, 3))
            value = jnp.where(comp == 3, norm, coords)
            rest = value - rounded(value)
            top = jnp.where(upper, value, rest)
            bottom = jnp.where(sub < 3, value, jnp.where(sub == 3, rest - rounded(rest), 1.0))
            right = jnp.concatenate([top, bottom], axis=0).astype(bf16)
            dots.append(jnp.dot(a_ref[i], right, preferred_element_type=f32))
        left = jnp.concatenate(lefts, axis=0).astype(bf16)
        return sides, left, dots

    def geometry(b, state):
        for n, s in enumerate(state[2]):
            g = jnp.maximum(s, 0.0)
            t = g * pl.reciprocal(1.125 - g, approx=True)
            f = (g * t) * (t + 3.0)
            hi = f.astype(bf16)
            f_ref[b % RING, n, 0] = hi
            f_ref[b % RING, n, 1] = (f - hi.astype(f32)).astype(bf16)

    def sums(b, state):
        sides, left, _ = state
        (hi0, lo0), (hi1, lo1) = [[f_ref[b % RING, n, h] for h in range(2)] for n in range(2)]
        own_rows = jnp.concatenate([w_ref[sides[0][1]], w_ref[sides[1][1]]], axis=0).astype(bf16)
        right_out = jnp.dot(
            jnp.concatenate([own_rows, own_rows], axis=1),
            jnp.concatenate(
                [jnp.concatenate([hi0, hi1], axis=1), jnp.concatenate([lo0, lo1], axis=1)], axis=0
            ),
            preferred_element_type=f32,
        )
        left_out = lax.dot_general(
            jnp.concatenate([left, left], axis=1),
            jnp.concatenate(
                [jnp.concatenate([hi0, lo0], axis=1), jnp.concatenate([hi1, lo1], axis=1)], axis=0
            ),
            (((1,), (1,)), ((), ())), preferred_element_type=f32,
        )
        return left_out, right_out

    def picked(total, mask, read):
        return [acc + jnp.where(mask, read(c), 0.0) for c, acc in enumerate(total)]

    def kept(b, state, outs, home, away):
        left_out, right_out = outs
        for n, (p, i, j, charge, w) in enumerate(state[0]):
            rows = slice(8 * n, 8 * n + 8)
            lanes = slice(n * CLUSTER, (n + 1) * CLUSTER)
            left = left_out[rows, lanes]
            right = right_out[rows, lanes]
            right = right + turned(right, 4)
            push_ref[b % RING, n, 0] = left + turned(left, 4)
            push_ref[b % RING, n, 1] = w * right[3:4] - charge * right

            def read(side, c):
                return push_ref[b % RING, n, side, pl.ds(c, 1), :]

            home = picked(home, sub == i, functools.partial(read, 0))
            for z in plan.order:
                if plan.starts[z] <= p < plan.ends[z]:
                    total = away.get(z, [jnp.zeros(tile, f32)] * 3)
                    away[z] = picked(total, sub == j - plan.rank[z] * clusters, functools.partial(read, 1))
        return home

    blocks = pair_count // 2
    batch_at = {}
    for n, batch in enumerate(plan.batches):
        batch_at.setdefault(plan.starts[batch[0]] // 2, []).append(n)
    last_of = {z: (plan.ends[z] - 1) // 2 for z in plan.order}
    done_at = [max(last_of[z] for z in batch) for batch in plan.batches]
    to_scalars.wait()

    for step in range(STEPS):
        states, outs = {}, {}
        home, away = [jnp.zeros(tile, f32)] * 4, {}
        pending, got = [], set()

        def send(n):
            for z in plan.batches[n]:
                force_copy(step, n, z).start()

        def settle(now):
            for n in list(pending):
                other = plan.twin[n]
                if now is None or now >= done_at[other] + HAND_BLOCKS:
                    arrived(some(hand_ref.at[step], n), recv_sem.at[2 * step + 1, other])
                    for r in range(plan.first[n], plan.first[n] + plan.size[n]):
                        force_ref[step, r] = force_ref[step, r] + hand_ref[step, r]
                    send(n)
                    pending.remove(n)

        def finished(n):
            if n and plan.second[n]:
                hand_copy(step, n).start()
            elif n in plan.twin:
                pending.append(n)
            elif n:
                send(n)

        for turn in range(blocks + 3):
            for n in batch_at.get(turn, []):
                arrive(step, n, got)
            if turn == 0:
                rows = [own_side(i) for i in range(clusters)]
                for i in range(clusters):
                    a_ref[i] = jnp.transpose(rows[i]).astype(bf16)
            if turn < blocks:
                states[turn] = prepare(turn)
            if 0 <= turn - 1 < blocks:
                geometry(turn - 1, states[turn - 1])
            if 0 <= turn - 2 < blocks:
                outs[turn - 2] = sums(turn - 2, states[turn - 2])
            if 0 <= turn - 3:
                now = turn - 3
                home = kept(now, states.pop(now), outs.pop(now), home, away)
                for z in plan.order:
                    if last_of[z] == now:
                        total = away.pop(z)
                        if z == own:
                            own_total = total
                            continue
                        for c in range(3):
                            rows = slice(c * clusters, (c + 1) * clusters)
                            force_ref[step, plan.rank[z], rows, :] = total[c][0:clusters]
                for n in range(len(plan.batches)):
                    if done_at[n] == now:
                        finished(n)
                settle(now)
        settle(None)

        ref = coords_ref(step)
        charge = first_ref[0, rows3 : rows3 + clusters, :]
        for c in range(3):
            rows = slice(c * clusters, (c + 1) * clusters)
            push = charge * (ref[0, rows, :] * home[3][0:clusters] - home[c][0:clusters])
            force_ref[step, 0, rows, :] = own_total[c][0:clusters] + push
        force = force_ref[step, 0]
        for n in plan.direct:
            arrived(some(land_ref.at[step], n), recv_sem.at[2 * step + 1, n])
            for r in range(plan.first[n], plan.first[n] + plan.size[n]):
                force = force + land_ref[step, r]
        velocity = vel_ref[...] + TIME_STEP * force
        coords = ref[0, 0:rows3, :] + TIME_STEP * velocity
        if step < STEPS - 1:
            vel_ref[...] = velocity
            later_ref[step, 0] = coords
            send_coords(step + 1)

    slot_ref[...] = jnp.zeros_like(slot_ref)
    for k in range(clusters):
        lanes = slice(k * CLUSTER, (k + 1) * CLUSTER)
        for c in range(3):
            r = c * clusters + k
            slot_ref[pl.ds(c, 1), lanes] = coords[r : r + 1]
            slot_ref[pl.ds(3 + c, 1), lanes] = velocity[r : r + 1]
            slot_ref[pl.ds(6 + c, 1), lanes] = force[r : r + 1]
    stacked = jnp.concatenate(split3(slot_ref[...]), axis=0)
    out = lax.dot_general(
        stacked, one_hot(atoms_ref, atom_count), (((1,), (1,)), ((), ())),
        preferred_element_type=f32,
    )
    atom = out[0:16] + out[16:32] + out[32:48]
    for c in range(3):
        x_out[c] = atom[c : c + 1]
        v_out[c] = atom[3 + c : 4 + c]
        f_out[c] = atom[6 + c : 7 + c]
    direct = sum(plan.size[n] for n in plan.direct)
    passed = sum(plan.size[n] for n in plan.twin if plan.second[n])
    for step in range(STEPS):
        for half, ref in enumerate((coords_ref(step), force_ref.at[step])):
            for way, count in enumerate((direct, passed)):
                if count:
                    arrived(ref.at[pl.ds(0, count)], send_sem.at[2 * step + half, way])


def shards(sizes, positions, velocities, charges, cluster_atoms, pair_list):
    zone = Zone(sizes)
    atom_count = positions.shape[-1]
    slots = cluster_atoms.shape[-1]
    pair_count = pair_list.shape[-1]
    clusters = slots // CLUSTER
    rows = 3 * clusters
    plan = Plan(zone, pair_count)
    f32, bf16, i32 = jnp.float32, jnp.bfloat16, jnp.int32
    x = positions.reshape(3, 1, atom_count)
    v = velocities.reshape(3, 1, atom_count)
    q = charges.reshape(1, atom_count)
    atoms = cluster_atoms.reshape(1, slots)
    pairs = pair_list.reshape(3, 1, pair_count)
    shape = jax.ShapeDtypeStruct((3, 1, atom_count), f32)
    block = (rows, CLUSTER)
    outs = pl.pallas_call(
        functools.partial(kernel, zone, plan),
        out_shape=(shape, shape, shape),
        in_specs=[VMEM] * 5,
        out_specs=(VMEM, VMEM, VMEM),
        scratch_shapes=[
            pltpu.VMEM((zone.count, 4 * clusters, CLUSTER), f32),
            pltpu.VMEM((STEPS - 1, zone.count) + block, f32),
            pltpu.VMEM((STEPS, zone.count) + block, f32),
            pltpu.VMEM((STEPS, zone.count) + block, f32),
            pltpu.VMEM((STEPS, zone.count) + block, f32),
            pltpu.VMEM(block, f32),
            pltpu.VMEM((16, slots), f32),
            pltpu.VMEM((zone.count * clusters, 8, CLUSTER), f32),
            pltpu.VMEM((SHIFTS, 8, CLUSTER), f32),
            pltpu.VMEM((clusters, CLUSTER, 16), bf16),
            pltpu.VMEM((clusters, 8, CLUSTER), f32),
            pltpu.VMEM((RING, 2, 2, CLUSTER, CLUSTER), bf16),
            pltpu.VMEM((RING, 2, 2, 8, CLUSTER), f32),
            pltpu.VMEM((8, pair_count), i32),
            pltpu.SMEM((8, pair_count), i32),
            pltpu.SemaphoreType.DMA((2 * STEPS, 2)),
            pltpu.SemaphoreType.DMA((2 * STEPS, len(plan.batches))),
            pltpu.SemaphoreType.DMA,
        ],
        compiler_params=pltpu.CompilerParams(collective_id=0, has_side_effects=True),
        name="leapfrog",
    )(pairs, x, v, q, atoms)
    return tuple(out.reshape(positions.shape) for out in outs)


def solution(mesh):
    spec3 = P(None, "gx", "gy", "gz", None)
    spec1 = P("gx", "gy", "gz", None)
    sizes = tuple(mesh.shape[axis] for axis in AXES)
    return jax.shard_map(
        functools.partial(shards, sizes),
        mesh=mesh,
        in_specs=(spec3, spec3, spec1, spec1, spec3),
        out_specs=(spec3, spec3, spec3),
        check_vma=False,
    )
```
